32 devices in a mesh: row: 16 (over z, x, core), col: 2 (over y).
Axes of the slice: x: 2, y: 2, z: 4, core: 2. Of those that a mesh axis runs over, the one named last changes fastest.
Arguments:
- embed_first: bfloat16 [768, 16384], P('col', 'row'), may hold values from -6 to 6
- embed_second: bfloat16 [768, 16384], P('row', 'col'), may hold values from -6 to 6
- corr_grad: float32 [16384, 16384], P('row', 'col'), may hold values from -0.046875 to 0.046875
Outputs:
- grad_first: bfloat16 [768, 16384], P('col', 'row')
- grad_second: bfloat16 [768, 16384], P('row', 'col')
The draws below stay inside these ranges and needn't reach their ends.
All inputs are finite; a program needn't handle non-finite values.
Results may differ from the reference program's by a relative error of at most 0.0065.
Values may be sent and summed in bfloat16 or wider, within the bound.
A program may use at most 128 MiB of HBM per device.

```python
import jax
import jax.numpy as jnp
from jax import lax

F = 16384
BATCH = 768


def levels(key, extent, cuts, low, high):
    def one(axis_at, shards_of):
        draws = jax.random.uniform(jax.random.fold_in(jax.random.fold_in(key, 6), axis_at), (shards_of,), jnp.float32, low / len(cuts), high / len(cuts))
        return jnp.repeat(jnp.exp(draws), extent[axis_at] // shards_of).reshape((-1,) + (1,) * (len(extent) - axis_at - 1))

    loudness = one(*cuts[0])
    for cut in cuts[1:]:
        loudness = loudness * one(*cut)
    return loudness


def noise(rng, shape, spread, limit, split=(), kind=jnp.bfloat16):
    gain = levels(rng, shape, split, -0.22, 0.18) if split else 1.0
    drawn = jax.random.normal(rng, shape, jnp.float32) * spread * gain
    return jnp.minimum(jnp.maximum(drawn, -limit), limit).astype(kind)


def setup_inputs(seed: int = 0) -> dict:
    splits = jax.random.split(jax.random.key(seed), 4)
    embed_first = noise(splits[0], (BATCH, F), 1.0, 6.0, ((0, 2), (1, 16)))
    embed_second = noise(splits[1], (BATCH, F), 1.0, 6.0, ((0, 16), (1, 2)))
    corr_grad = noise(splits[2], (F, F), F ** -0.5, 0.046875, ((0, 16), (1, 2)), jnp.float32)
    return {"embed_first": embed_first, "embed_second": embed_second, "corr_grad": corr_grad}


def reference(embed_first, embed_second, corr_grad):
    low_grad = corr_grad.astype(jnp.bfloat16)
    grad_first = lax.dot_general(embed_second, low_grad, (((1,), (1,)), ((), ())), preferred_element_type=jnp.float32)
    grad_second = jnp.dot(embed_first, low_grad, preferred_element_type=jnp.float32)
    return grad_first.astype(jnp.bfloat16), grad_second.astype(jnp.bfloat16)
```

```python
import functools

import jax
import jax.numpy as jnp
from jax import lax
from jax.experimental import pallas as pl
from jax.experimental.pallas import tpu as pltpu
from jax.sharding import PartitionSpec as P

OWN, OTHER, GATHER, SUMS, FIRST = range(5)
STEPS = (
    (OWN, 0, 0, 0), (GATHER, 0, 1, 0), (OWN, 0, 0, 1), (GATHER, 1, 0, 2), (GATHER, 0, 1, 1), (OTHER, 0, 0, 0),
    (OTHER, 0, 0, 1), (GATHER, 0, 1, 2), (GATHER, 1, 0, 3), (SUMS, 3, 0, 0), (SUMS, 3, 1, 2), (SUMS, 3, 1, 1),
    (SUMS, 3, 0, 1), (GATHER, 1, 1, 2), (SUMS, 3, 1, 0), (GATHER, 1, 0, 1), (OTHER, 1, 0, 0),
    (GATHER, 0, 1, 3), (SUMS, 3, 1, 3), (OTHER, 1, 0, 1), (SUMS, 3, 0, 2), (GATHER, 2, 0, 2),
    (GATHER, 1, 1, 1), (GATHER, 1, 1, 3), (SUMS, 2, 1, 3), (GATHER, 2, 0, 3), (GATHER, 1, 0, 0),
    (SUMS, 3, 0, 3), (GATHER, 1, 1, 0), (SUMS, 1, 1, 3), (GATHER, 3, 0, 2), (SUMS, 2, 0, 1), (SUMS, 2, 1, 0),
    (SUMS, 2, 1, 1), (FIRST, 1, 0, 0), (SUMS, 2, 1, 2), (SUMS, 2, 0, 3), (GATHER, 2, 0, 0), (SUMS, 2, 0, 0),
    (GATHER, 2, 0, 1), (GATHER, 2, 1, 3), (FIRST, 0, 0, 0), (GATHER, 3, 0, 0), (GATHER, 2, 1, 2),
    (GATHER, 3, 0, 3), (GATHER, 2, 1, 0), (GATHER, 2, 1, 1), (SUMS, 1, 1, 2), (SUMS, 1, 1, 0),
    (GATHER, 3, 0, 1), (SUMS, 1, 1, 1), (GATHER, 3, 1, 2), (SUMS, 1, 0, 3), (FIRST, 2, 0, 0),
    (GATHER, 3, 1, 1), (SUMS, 2, 0, 2), (SUMS, 0, 1, 2), (SUMS, 1, 0, 0), (GATHER, 3, 1, 3),
    (GATHER, 3, 1, 0), (SUMS, 0, 1, 0), (SUMS, 0, 1, 3), (FIRST, 3, 0, 0), (SUMS, 1, 0, 2), (SUMS, 1, 0, 1),
    (SUMS, 0, 1, 1),
)
FIRST_SHARE = 0.4
TILE = 256
SLOTS = 3


def cuts(fj):
    unit = fj // 256
    short = round(unit * FIRST_SHARE)
    widths = [(True, short), (True, short), (False, unit - short), (False, unit - short)]
    out, at = [], 0
    for kind, w in widths:
        out.append((kind, at, w * 128))
        at += w * 128
    return out


def slots_of(side):
    return 1 if side == 2 else side + 1


def kernel(
    a_side, b_side, cols,
    e1_hbm, e2_hbm, g_ref, o1_ref, o2_ref,
    e1_ref, e1x, e2x, gb, p2, s2, rb_short, rb_long, acc, t1s, t1r, gt,
    in_sem, g_sem, e1_send, e1_recv, ag_send, ag_recv, sib_send, sib_recv,
    d2d_send, d2d_recv, rs_send, rs_recv_short, rs_recv_long, t1_send, t1_recv,
):
    chips = a_side * b_side
    block, fj = e2_hbm.shape
    rows, fi = e1_hbm.shape
    share = chips // cols
    bf16, f32 = jnp.bfloat16, jnp.float32
    pieces = cuts(fj)
    sides = {"a": a_side, "b": b_side}

    me = lax.axis_index("row")
    my_col = lax.axis_index("col")
    chip, core = me // 2, me % 2
    other = 1 - core
    here = {"a": chip // b_side, "b": chip % b_side}
    sibling = chip * 2 + other

    def at_offset(da, db):
        return chip + da * b_side + db

    def neighbour(axis, sign):
        return (chip + sign * (b_side if axis == "a" else 1)) * 2 + core

    def inside(axis, d):
        where = here[axis] + d
        return jnp.logical_and(where >= 0, where < sides[axis])

    def both_inside(da, db):
        return jnp.logical_and(inside("a", da), inside("b", db))

    def piece(k):
        return pl.ds(pieces[k][1], pieces[k][2])

    def remote(src, dst, send, recv, **to):
        return pltpu.make_async_remote_copy(
            src_ref=src, dst_ref=dst, send_sem=send, recv_sem=recv,
            device_id=to, device_id_type=pl.DeviceIdType.MESH,
        )

    WAYS = (("a", 1), ("a", -1), ("b", 1), ("b", -1))

    inputs = (
        pltpu.make_async_copy(e2_hbm, e2x.at[chip, core], in_sem.at[0]),
        pltpu.make_async_copy(e1_hbm, e1_ref, in_sem.at[1]),
    )
    for copy in inputs:
        copy.start()

    barrier = pltpu.get_barrier_semaphore()
    for axis, sign in WAYS:
        @pl.when(inside(axis, sign))
        def _():
            pl.semaphore_signal(
                barrier, inc=1, device_id={"row": neighbour(axis, sign)}, device_id_type=pl.DeviceIdType.MESH
            )
    pl.semaphore_signal(barrier, inc=1, device_id={"row": sibling}, device_id_type=pl.DeviceIdType.MESH)
    for off in range(1, cols):
        pl.semaphore_signal(
            barrier, inc=1, device_id={"col": (my_col + off) % cols}, device_id_type=pl.DeviceIdType.MESH
        )
    peers = sum(inside(*way).astype(jnp.int32) for way in WAYS)
    pl.semaphore_wait(barrier, peers + cols)

    def block_copy(da, db, k, way):
        src_chip = at_offset(da, db)
        dst = e2x.at[src_chip, core, :, piece(k)]
        return remote(
            dst, dst, ag_send.at[src_chip, k, way], ag_recv.at[src_chip, k], row=neighbour(*WAYS[way])
        )

    def sibling_copy(da, db, k):
        src_chip = at_offset(da, db)
        dst = e2x.at[src_chip, core, :, piece(k)]
        return remote(dst, dst, sib_send.at[src_chip, k], sib_recv.at[src_chip, k], row=sibling)

    def onward(da, db, k):
        first, second = ("b", "a") if pieces[k][0] else ("a", "b")
        d = {"a": da, "b": db}
        for way, (axis, sign) in enumerate(WAYS):
            if axis == second:
                if d[second] * sign <= 0:
                    yield way
            elif d[second] == 0 and d[first] * sign <= 0:
                yield way

    def send_on(da, db, k):
        for way in onward(da, db, k):
            @pl.when(inside(*WAYS[way]))
            def _():
                block_copy(da, db, k, way).start()

    near, late = (0, 1), (2, 3)

    def sides_of(d):
        return (d, -d) if d else (0,)

    def gather(d, side, k):
        for db in across if side else (0,):
            for da in sides_of(d):
                @pl.when(both_inside(da, db))
                def _():
                    block_copy(da, db, k, 0).wait_recv()
                    send_on(da, db, k)
                    sibling_copy(da, db, k).start()

    across = sorted((db for db in range(1 - b_side, b_side) if db), key=abs)

    inputs[0].wait()
    for k in late + near:
        for way in onward(0, 0, k):
            if WAYS[way][0] == "a":
                @pl.when(inside(*WAYS[way]))
                def _():
                    block_copy(0, 0, k, way).start()
    for k in near + late:
        for way in onward(0, 0, k):
            if WAYS[way][0] == "b":
                @pl.when(inside(*WAYS[way]))
                def _():
                    block_copy(0, 0, k, way).start()

    parts = max(share // b_side, 1)
    part_chips, part_rows = share // parts, rows // parts

    def part_of(col, q):
        return jnp.where(col * 2 < cols, q, parts - 1 - q)

    def e1_copy(off, q):
        at = pl.ds(pl.multiple_of(part_of(my_col, q) * part_rows, part_rows), part_rows)
        return remote(
            e1_ref.at[at], e1x.at[off - 1, at], e1_send.at[off - 1, q], e1_recv.at[off - 1, q],
            col=(my_col + off) % cols,
        )

    def e1_arrival(off, q):
        from_col = (my_col - off + cols) % cols
        at = pl.ds(pl.multiple_of(part_of(from_col, q) * part_rows, part_rows), part_rows)
        return remote(
            e1_ref.at[at], e1x.at[off - 1, at], e1_send.at[off - 1, q], e1_recv.at[off - 1, q], col=from_col
        )

    inputs[1].wait()
    for q in range(parts):
        for off in range(1, cols):
            e1_copy(off, q).start()

    def load(n):
        slot = n % SLOTS
        return pltpu.make_async_copy(
            g_ref.at[:, pl.ds(pl.multiple_of(n * TILE, TILE), TILE)], gt.at[slot], g_sem.at[slot]
        )

    tiles = fj // TILE
    for n in range(SLOTS):
        load(n).start()
    for k in near + late:
        sibling_copy(0, 0, k).start()

    def first_pass(n, carry):
        load(n).wait()
        at = pl.ds(pl.multiple_of(n * TILE, TILE), TILE)
        low = gt[n % SLOTS].astype(bf16)
        gb[:, at] = low

        @pl.when(n + SLOTS < tiles)
        def _():
            load(n + SLOTS).start()

        terms = jnp.dot(e1_ref[...], low, preferred_element_type=f32).astype(bf16)
        p2[pl.ds(my_col * share, share), :, :, at] = terms.reshape(share, 2, block, TILE)
        return carry

    def next_pass(off, q, wide):
        from_col = (my_col - off + cols) % cols
        part = part_of(from_col, q)
        left = pl.ds(pl.multiple_of(part * part_rows, part_rows), part_rows)
        to = pl.ds(from_col * share + part * part_chips, part_chips)

        def body(n, carry):
            at = pl.ds(pl.multiple_of(n * wide, wide), wide)
            terms = jnp.dot(e1x[off - 1, left], gb[:, at], preferred_element_type=f32).astype(bf16)
            p2[to, :, :, at] = terms.reshape(part_chips, 2, block, wide)
            return carry

        return body

    def d2d_copy(off, q, h):
        from_col = (my_col - off + cols) % cols
        if off:
            chunk = pl.ds(from_col * share + part_of(from_col, q) * part_chips, part_chips)
        else:
            chunk = pl.ds(from_col * share, share)
        at = pl.ds(h * (fj // 2), fj // 2)
        return remote(
            p2.at[chunk, other, :, at], s2.at[chunk, :, at],
            d2d_send.at[off, q, h], d2d_recv.at[off, q, h], row=sibling,
        )

    wide = 512

    def own_terms(h):
        lax.fori_loop(h * tiles // 2, (h + 1) * tiles // 2, first_pass, 0)
        d2d_copy(0, 0, h).start()

    def other_terms(q, h):
        for off in range(1, cols):
            if h == 0:
                e1_arrival(off, q).wait_recv()
            lax.fori_loop(h * fj // wide // 2, (h + 1) * fj // wide // 2, next_pass(off, q, wide), 0)
            d2d_copy(off, q, h).start()

    def terms_ready(q):
        for off in range(0 if q == 0 else 1, cols):
            for h in range(2):
                d2d_copy(off, q, h).wait_recv()

    def sum_slot(k, axis, sign, to):
        short = pieces[k][0]
        first, second = ("a", "b") if short else ("b", "a")
        place = to["a"] if axis == "a" else to["b"]
        slot = 0 if sides[axis] == 2 else (place + 1 if sign > 0 else place)
        if axis == first:
            slot = to[second] * slots_of(sides[first]) + slot
        else:
            slot = sides[second] * slots_of(sides[first]) + slot
        start = pieces[k][1] if short else pieces[k][1] - pieces[2][1]
        buf = rb_short if short else rb_long
        sem = rs_recv_short if short else rs_recv_long
        return buf.at[slot, :, pl.ds(start, pieces[k][2])], sem.at[slot, k % 2]

    def place_of(da, db):
        return {"a": here["a"] + da, "b": here["b"] + db}

    def way_out(da, db, k):
        first, second = ("a", "b") if pieces[k][0] else ("b", "a")
        d = {"a": da, "b": db}
        axis = first if d[first] else second
        return axis, (1 if d[axis] > 0 else -1)

    def sum_copy(da, db, k):
        axis, sign = way_out(da, db, k)
        to_chip = at_offset(da, db)
        dst, sem = sum_slot(k, axis, sign, place_of(da, db))
        return remote(
            p2.at[to_chip, core, :, piece(k)], dst, rs_send.at[to_chip, k], sem, row=neighbour(axis, sign)
        )

    def arrivals(da, db, k):
        first, second = ("a", "b") if pieces[k][0] else ("b", "a")
        d = {"a": da, "b": db}
        out = []
        for sign in (1, -1):
            if d[first] * sign >= 0:
                out.append((first, sign))
        if d[first] == 0:
            for sign in (1, -1):
                if d[second] * sign >= 0:
                    out.append((second, sign))
        return out

    def sum_of(da, db, k):
        at = piece(k)
        to_chip = at_offset(da, db)
        kept = acc.at[:, pl.ds(0, pieces[k][2])]
        kept[...] = p2[to_chip, core, :, at].astype(f32) + s2[to_chip, :, at].astype(f32)
        for axis, sign in arrivals(da, db, k):
            @pl.when(inside(axis, -sign))
            def _():
                buf, sem = sum_slot(k, axis, sign, place_of(da, db))
                remote(buf, buf, rs_send.at[0, k], sem, row=sibling).wait_recv()
                kept[...] += buf[...].astype(f32)
        return kept[...].astype(bf16)

    def send_sums(d, side, k):
        for db in reversed(across) if side else (0,):
            for da in sides_of(d):
                @pl.when(both_inside(da, db))
                def _():
                    p2[at_offset(da, db), core, :, piece(k)] = sum_of(da, db, k)
                    sum_copy(da, db, k).start()

    unit = min(share, b_side)
    unit_rows = unit * 2 * block

    def t1_copy(off, slot):
        at = pl.ds(pl.multiple_of(slot * unit_rows, unit_rows), unit_rows)
        return remote(
            t1s.at[off - 1, at], t1r.at[off - 1, at], t1_send.at[off - 1, slot], t1_recv.at[off - 1, slot],
            col=(my_col + off) % cols,
        )

    def keep(n, slot):
        return gt.at[n // 2, pl.ds(pl.multiple_of(n % 2 * rows + slot * unit_rows, unit_rows), unit_rows)]

    def first_terms(d):
        for da in sides_of(d):
            for db in range(1 - b_side, b_side):
                @pl.when(both_inside(da, db))
                def _():
                    for k in range(4):
                        sibling_copy(da, db, k).wait_recv()

        def one_side(s, carry):
            plane = here["a"] + d * (1 - 2 * s)

            @pl.when(jnp.logical_and(plane >= 0, plane < a_side))
            def _():
                for g in range(b_side // unit):
                    chunk = plane * (b_side // unit) + g
                    first_chip = chunk * unit
                    off = (first_chip // share - my_col + cols) % cols
                    slot = first_chip % share // unit

                    def body(n, carry):
                        left_side = e2x[pl.ds(first_chip, unit)].reshape(unit_rows, fj)
                        part = gb[pl.ds(pl.multiple_of(n * TILE, TILE), TILE), :]
                        terms = lax.dot_general(
                            left_side, part, (((1,), (1,)), ((), ())), preferred_element_type=f32
                        )

                        @pl.when(off == 0)
                        def _():
                            keep(n, slot)[...] = terms

                        @pl.when(off != 0)
                        def _():
                            at = pl.ds(pl.multiple_of(slot * unit_rows, unit_rows), unit_rows)
                            to = pl.ds(pl.multiple_of(n * TILE, TILE), TILE)
                            t1s[off - 1, at, to] = terms.astype(bf16)

                        return carry

                    lax.fori_loop(0, fi // TILE, body, 0)

                    @pl.when(off != 0)
                    def _():
                        t1_copy(off, slot).start()

            return carry

        lax.fori_loop(0, 2 if d else 1, one_side, 0)

    ready = 0
    for kind, d, side, k in STEPS:
        if kind == OWN:
            own_terms(k)
        elif kind == OTHER:
            for q in (0,) if d == 0 else range(1, parts):
                other_terms(q, k)
        elif kind == GATHER:
            gather(d, side, k)
        elif kind == SUMS:
            for q in range(ready, 1 if d == a_side - 1 else parts):
                terms_ready(q)
                ready = q + 1
            send_sums(d, side, k)
        else:
            first_terms(d)

    def last_wait(kept):
        for da in range(1 - a_side, a_side):
            for db in range(1 - b_side, b_side):
                for k in range(4):
                    axis, _ = way_out(da, db, k)
                    recent = abs(da) == 1 and axis == "a" or da == 0
                    if recent == kept and (da, db) != (0, 0):
                        @pl.when(both_inside(da, db))
                        def _():
                            sum_copy(da, db, k).wait_send()

    for da in range(1 - a_side, a_side):
        for db in range(1 - b_side, b_side):
            @pl.when(both_inside(da, db))
            def _():
                for k in range(4):
                    for way in onward(da, db, k):
                        @pl.when(inside(*WAYS[way]))
                        def _():
                            block_copy(da, db, k, way).wait_send()
                    sibling_copy(da, db, k).wait_send()
    for off in range(cols):
        for q in range(parts if off else 1):
            for h in range(2):
                d2d_copy(off, q, h).wait_send()
    for off in range(1, cols):
        for q in range(parts):
            e1_copy(off, q).wait_send()
    last_wait(False)

    for off in range(1, cols):
        for slot in range(share // unit):
            t1_copy(off, slot).wait_recv()

    def out_body(n, carry):
        at = pl.ds(pl.multiple_of(n * TILE, TILE), TILE)
        for slot in range(share // unit):
            these = pl.ds(slot * unit_rows, unit_rows)
            total = keep(n, slot)[...]
            for off in range(1, cols):
                total += t1r[off - 1, these, at].astype(f32)
            o1_ref[these, at] = total.astype(bf16)
        return carry

    lax.fori_loop(0, fi // TILE, out_body, 0)

    for k in late + near:
        o2_ref[:, piece(k)] = sum_of(0, 0, k)

    last_wait(True)
    for off in range(1, cols):
        for slot in range(share // unit):
            t1_copy(off, slot).wait_send()


def local(rows_size, cols, e1, e2, g):
    chips = rows_size // 2
    a_side = 4
    b_side = chips // a_side
    block, fj = e2.shape
    rows, fi = e1.shape
    bf16 = jnp.bfloat16
    vmem, hbm = pl.BlockSpec(memory_space=pltpu.VMEM), pl.BlockSpec(memory_space=pl.ANY)
    dma = pltpu.SemaphoreType.DMA
    pieces = cuts(fj)
    share = chips // cols
    parts, slots = max(share // b_side, 1), share // min(share, b_side)
    short, long = 2 * pieces[0][2], 2 * pieces[2][2]
    short_slots = b_side * slots_of(a_side) + slots_of(b_side)
    long_slots = a_side * slots_of(b_side) + slots_of(a_side)
    return pl.pallas_call(
        functools.partial(kernel, a_side, b_side, cols),
        out_shape=(jax.ShapeDtypeStruct(e1.shape, bf16), jax.ShapeDtypeStruct(e2.shape, bf16)),
        in_specs=[hbm, hbm, hbm],
        out_specs=(vmem, vmem),
        scratch_shapes=[
            pltpu.VMEM((rows, fi), bf16),
            pltpu.VMEM((cols - 1, rows, fi), bf16),
            pltpu.VMEM((chips, 2, block, fj), bf16),
            pltpu.VMEM((fi, fj), bf16),
            pltpu.VMEM((chips, 2, block, fj), bf16),
            pltpu.VMEM((chips, block, fj), bf16),
            pltpu.VMEM((short_slots, block, short), bf16),
            pltpu.VMEM((long_slots, block, long), bf16),
            pltpu.VMEM((block, max(short, long) // 2), jnp.float32),
            pltpu.VMEM((cols - 1, rows, fi), bf16),
            pltpu.VMEM((cols - 1, rows, fi), bf16),
            pltpu.VMEM((SLOTS, fi, TILE), jnp.float32),
            dma((2,)), dma((SLOTS,)),
            dma((cols - 1, parts)), dma((cols - 1, parts)),
            dma((chips, 4, 4)), dma((chips, 4)),
            dma((chips, 4)), dma((chips, 4)),
            dma((cols, parts, 2)), dma((cols, parts, 2)),
            dma((chips, 4)), dma((short_slots, 2)), dma((long_slots, 2)),
            dma((cols - 1, slots)), dma((cols - 1, slots)),
        ],
        compiler_params=pltpu.CompilerParams(
            collective_id=0, has_side_effects=True, vmem_limit_bytes=67043328
        ),
    )(e1, e2, g)


def solution(mesh):
    return jax.shard_map(
        functools.partial(local, mesh.shape["row"], mesh.shape["col"]),
        mesh=mesh,
        in_specs=(P("col", "row"), P("row", "col"), P("row", "col")),
        out_specs=(P("col", "row"), P("row", "col")),
        check_vma=False,
    )
```

```python
import functools

import jax
import jax.numpy as jnp
from jax import lax
from jax.experimental import pallas as pl
from jax.experimental.pallas import tpu as pltpu
from jax.sharding import PartitionSpec as P

OWN, OTHER, GATHER, SUMS, FIRST = range(5)
STEPS = (
    (OWN, 0, 0, 0), (GATHER, 0, 1, 0), (OWN, 0, 0, 1), (GATHER, 1, 0, 2), (GATHER, 0, 1, 1), (OTHER, 0, 0, 0),
    (OTHER, 0, 0, 1), (GATHER, 0, 1, 2), (GATHER, 1, 0, 3), (SUMS, 3, 0, 0), (SUMS, 3, 1, 2), (SUMS, 3, 1, 1),
    (SUMS, 3, 0, 1), (GATHER, 1, 1, 2), (SUMS, 3, 1, 0), (GATHER, 1, 0, 1), (OTHER, 1, 0, 0),
    (GATHER, 0, 1, 3), (SUMS, 3, 1, 3), (OTHER, 1, 0, 1), (SUMS, 3, 0, 2), (GATHER, 2, 0, 2),
    (GATHER, 1, 1, 1), (GATHER, 1, 1, 3), (SUMS, 2, 1, 3), (GATHER, 2, 0, 3), (GATHER, 1, 0, 0),
    (SUMS, 3, 0, 3), (GATHER, 1, 1, 0), (SUMS, 1, 1, 3), (GATHER, 3, 0, 2), (SUMS, 2, 0, 1), (SUMS, 2, 1, 0),
    (SUMS, 2, 1, 1), (FIRST, 1, 0, 0), (SUMS, 2, 1, 2), (SUMS, 2, 0, 3), (GATHER, 2, 0, 0), (SUMS, 2, 0, 0),
    (GATHER, 2, 0, 1), (GATHER, 2, 1, 3), (FIRST, 0, 0, 0), (GATHER, 3, 0, 0), (GATHER, 2, 1, 2),
    (GATHER, 3, 0, 3), (GATHER, 2, 1, 0), (GATHER, 2, 1, 1), (SUMS, 1, 1, 2), (SUMS, 1, 1, 0),
    (GATHER, 3, 0, 1), (SUMS, 1, 1, 1), (GATHER, 3, 1, 2), (SUMS, 1, 0, 3), (FIRST, 2, 0, 0),
    (GATHER, 3, 1, 1), (SUMS, 2, 0, 2), (SUMS, 0, 1, 2), (SUMS, 1, 0, 0), (GATHER, 3, 1, 3),
    (GATHER, 3, 1, 0), (SUMS, 0, 1, 0), (SUMS, 0, 1, 3), (FIRST, 3, 0, 0), (SUMS, 1, 0, 2), (SUMS, 1, 0, 1),
    (SUMS, 0, 1, 1),
)
FIRST_SHARE = 0.4
TILE = 256
SLOTS = 3


def cuts(fj):
    unit = fj // 256
    short = round(unit * FIRST_SHARE)
    widths = [(True, short), (True, short), (False, unit - short), (False, unit - short)]
    out, at = [], 0
    for kind, w in widths:
        out.append((kind, at, w * 128))
        at += w * 128
    return out


def slots_of(side):
    return 1 if side == 2 else side + 1


def kernel(
    a_side, b_side, cols,
    e1_hbm, e2_hbm, g_ref, o1_hbm, o2_hbm,
    o1_ref, o2_ref,    e1_ref, e1x, e2x, gb, p2, s2, rb_short, rb_long, acc, t1s, t1r, gt,
    in_sem, out_sem, g_sem, e1_send, e1_recv, ag_send, ag_recv, sib_send, sib_recv,
    d2d_send, d2d_recv, rs_send, rs_recv_short, rs_recv_long, t1_send, t1_recv,
):
    chips = a_side * b_side
    block, fj = e2_hbm.shape
    rows, fi = e1_hbm.shape
    share = chips // cols
    bf16, f32 = jnp.bfloat16, jnp.float32
    pieces = cuts(fj)
    sides = {"a": a_side, "b": b_side}

    me = lax.axis_index("row")
    my_col = lax.axis_index("col")
    chip, core = me // 2, me % 2
    other = 1 - core
    here = {"a": chip // b_side, "b": chip % b_side}
    sibling = chip * 2 + other

    def at_offset(da, db):
        return chip + da * b_side + db

    def neighbour(axis, sign):
        return (chip + sign * (b_side if axis == "a" else 1)) * 2 + core

    def inside(axis, d):
        where = here[axis] + d
        return jnp.logical_and(where >= 0, where < sides[axis])

    def both_inside(da, db):
        return jnp.logical_and(inside("a", da), inside("b", db))

    def piece(k):
        return pl.ds(pieces[k][1], pieces[k][2])

    def remote(src, dst, send, recv, **to):
        return pltpu.make_async_remote_copy(
            src_ref=src, dst_ref=dst, send_sem=send, recv_sem=recv,
            device_id=to, device_id_type=pl.DeviceIdType.MESH,
        )

    WAYS = (("a", 1), ("a", -1), ("b", 1), ("b", -1))

    inputs = (
        pltpu.make_async_copy(e2_hbm, e2x.at[chip, core], in_sem.at[0]),
        pltpu.make_async_copy(e1_hbm, e1_ref, in_sem.at[1]),
    )
    for copy in inputs:
        copy.start()

    barrier = pltpu.get_barrier_semaphore()
    for axis, sign in WAYS:
        @pl.when(inside(axis, sign))
        def _():
            pl.semaphore_signal(
                barrier, inc=1, device_id={"row": neighbour(axis, sign)}, device_id_type=pl.DeviceIdType.MESH
            )
    pl.semaphore_signal(barrier, inc=1, device_id={"row": sibling}, device_id_type=pl.DeviceIdType.MESH)
    for off in range(1, cols):
        pl.semaphore_signal(
            barrier, inc=1, device_id={"col": (my_col + off) % cols}, device_id_type=pl.DeviceIdType.MESH
        )
    peers = sum(inside(*way).astype(jnp.int32) for way in WAYS)
    pl.semaphore_wait(barrier, peers + cols)

    def block_copy(da, db, k, way):
        src_chip = at_offset(da, db)
        dst = e2x.at[src_chip, core, :, piece(k)]
        return remote(
            dst, dst, ag_send.at[src_chip, k, way], ag_recv.at[src_chip, k], row=neighbour(*WAYS[way])
        )

    def sibling_copy(da, db, k):
        src_chip = at_offset(da, db)
        dst = e2x.at[src_chip, core, :, piece(k)]
        return remote(dst, dst, sib_send.at[src_chip, k], sib_recv.at[src_chip, k], row=sibling)

    def onward(da, db, k):
        first, second = ("b", "a") if pieces[k][0] else ("a", "b")
        d = {"a": da, "b": db}
        for way, (axis, sign) in enumerate(WAYS):
            if axis == second:
                if d[second] * sign <= 0:
                    yield way
            elif d[second] == 0 and d[first] * sign <= 0:
                yield way

    def send_on(da, db, k):
        for way in onward(da, db, k):
            @pl.when(inside(*WAYS[way]))
            def _():
                block_copy(da, db, k, way).start()

    near, late = (0, 1), (2, 3)

    def sides_of(d):
        return (d, -d) if d else (0,)

    def gather(d, side, k):
        for db in across if side else (0,):
            for da in sides_of(d):
                @pl.when(both_inside(da, db))
                def _():
                    block_copy(da, db, k, 0).wait_recv()
                    send_on(da, db, k)
                    sibling_copy(da, db, k).start()

    across = sorted((db for db in range(1 - b_side, b_side) if db), key=abs)

    inputs[0].wait()
    for k in late + near:
        for way in onward(0, 0, k):
            if WAYS[way][0] == "a":
                @pl.when(inside(*WAYS[way]))
                def _():
                    block_copy(0, 0, k, way).start()
    for k in near + late:
        for way in onward(0, 0, k):
            if WAYS[way][0] == "b":
                @pl.when(inside(*WAYS[way]))
                def _():
                    block_copy(0, 0, k, way).start()

    parts = max(share // b_side, 1)
    part_chips, part_rows = share // parts, rows // parts

    def part_of(col, q):
        return jnp.where(col * 2 < cols, q, parts - 1 - q)

    def e1_copy(off, q):
        at = pl.ds(pl.multiple_of(part_of(my_col, q) * part_rows, part_rows), part_rows)
        return remote(
            e1_ref.at[at], e1x.at[off - 1, at], e1_send.at[off - 1, q], e1_recv.at[off - 1, q],
            col=(my_col + off) % cols,
        )

    def e1_arrival(off, q):
        from_col = (my_col - off + cols) % cols
        at = pl.ds(pl.multiple_of(part_of(from_col, q) * part_rows, part_rows), part_rows)
        return remote(
            e1_ref.at[at], e1x.at[off - 1, at], e1_send.at[off - 1, q], e1_recv.at[off - 1, q], col=from_col
        )

    inputs[1].wait()
    for q in range(parts):
        for off in range(1, cols):
            e1_copy(off, q).start()

    def load(n):
        slot = n % SLOTS
        return pltpu.make_async_copy(
            g_ref.at[:, pl.ds(pl.multiple_of(n * TILE, TILE), TILE)], gt.at[slot], g_sem.at[slot]
        )

    tiles = fj // TILE
    for n in range(SLOTS):
        load(n).start()
    for k in near + late:
        sibling_copy(0, 0, k).start()

    def first_pass(n, carry):
        load(n).wait()
        at = pl.ds(pl.multiple_of(n * TILE, TILE), TILE)
        low = gt[n % SLOTS].astype(bf16)
        gb[:, at] = low

        @pl.when(n + SLOTS < tiles)
        def _():
            load(n + SLOTS).start()

        terms = jnp.dot(e1_ref[...], low, preferred_element_type=f32).astype(bf16)
        p2[pl.ds(my_col * share, share), :, :, at] = terms.reshape(share, 2, block, TILE)
        return carry

    def next_pass(off, q, wide):
        from_col = (my_col - off + cols) % cols
        part = part_of(from_col, q)
        left = pl.ds(pl.multiple_of(part * part_rows, part_rows), part_rows)
        to = pl.ds(from_col * share + part * part_chips, part_chips)

        def body(n, carry):
            at = pl.ds(pl.multiple_of(n * wide, wide), wide)
            terms = jnp.dot(e1x[off - 1, left], gb[:, at], preferred_element_type=f32).astype(bf16)
            p2[to, :, :, at] = terms.reshape(part_chips, 2, block, wide)
            return carry

        return body

    def d2d_copy(off, q, h):
        from_col = (my_col - off + cols) % cols
        if off:
            chunk = pl.ds(from_col * share + part_of(from_col, q) * part_chips, part_chips)
        else:
            chunk = pl.ds(from_col * share, share)
        at = pl.ds(h * (fj // 2), fj // 2)
        return remote(
            p2.at[chunk, other, :, at], s2.at[chunk, :, at],
            d2d_send.at[off, q, h], d2d_recv.at[off, q, h], row=sibling,
        )

    wide = 512

    def own_terms(h):
        lax.fori_loop(h * tiles // 2, (h + 1) * tiles // 2, first_pass, 0)
        d2d_copy(0, 0, h).start()

    def other_terms(q, h):
        for off in range(1, cols):
            if h == 0:
                e1_arrival(off, q).wait_recv()
            lax.fori_loop(h * fj // wide // 2, (h + 1) * fj // wide // 2, next_pass(off, q, wide), 0)
            d2d_copy(off, q, h).start()

    def terms_ready(q):
        for off in range(0 if q == 0 else 1, cols):
            for h in range(2):
                d2d_copy(off, q, h).wait_recv()

    def sum_slot(k, axis, sign, to):
        short = pieces[k][0]
        first, second = ("a", "b") if short else ("b", "a")
        place = to["a"] if axis == "a" else to["b"]
        slot = 0 if sides[axis] == 2 else (place + 1 if sign > 0 else place)
        if axis == first:
            slot = to[second] * slots_of(sides[first]) + slot
        else:
            slot = sides[second] * slots_of(sides[first]) + slot
        start = pieces[k][1] if short else pieces[k][1] - pieces[2][1]
        buf = rb_short if short else rb_long
        sem = rs_recv_short if short else rs_recv_long
        return buf.at[slot, :, pl.ds(start, pieces[k][2])], sem.at[slot, k % 2]

    def place_of(da, db):
        return {"a": here["a"] + da, "b": here["b"] + db}

    def way_out(da, db, k):
        first, second = ("a", "b") if pieces[k][0] else ("b", "a")
        d = {"a": da, "b": db}
        axis = first if d[first] else second
        return axis, (1 if d[axis] > 0 else -1)

    def sum_copy(da, db, k):
        axis, sign = way_out(da, db, k)
        to_chip = at_offset(da, db)
        dst, sem = sum_slot(k, axis, sign, place_of(da, db))
        return remote(
            p2.at[to_chip, core, :, piece(k)], dst, rs_send.at[to_chip, k], sem, row=neighbour(axis, sign)
        )

    def arrivals(da, db, k):
        first, second = ("a", "b") if pieces[k][0] else ("b", "a")
        d = {"a": da, "b": db}
        out = []
        for sign in (1, -1):
            if d[first] * sign >= 0:
                out.append((first, sign))
        if d[first] == 0:
            for sign in (1, -1):
                if d[second] * sign >= 0:
                    out.append((second, sign))
        return out

    def sum_of(da, db, k):
        at = piece(k)
        to_chip = at_offset(da, db)
        kept = acc.at[:, pl.ds(0, pieces[k][2])]
        kept[...] = p2[to_chip, core, :, at].astype(f32) + s2[to_chip, :, at].astype(f32)
        for axis, sign in arrivals(da, db, k):
            @pl.when(inside(axis, -sign))
            def _():
                buf, sem = sum_slot(k, axis, sign, place_of(da, db))
                remote(buf, buf, rs_send.at[0, k], sem, row=sibling).wait_recv()
                kept[...] += buf[...].astype(f32)
        return kept[...].astype(bf16)

    def send_sums(d, side, k):
        for db in reversed(across) if side else (0,):
            for da in sides_of(d):
                @pl.when(both_inside(da, db))
                def _():
                    p2[at_offset(da, db), core, :, piece(k)] = sum_of(da, db, k)
                    sum_copy(da, db, k).start()

    unit = min(share, b_side)
    unit_rows = unit * 2 * block

    def t1_copy(off, slot):
        at = pl.ds(pl.multiple_of(slot * unit_rows, unit_rows), unit_rows)
        return remote(
            t1s.at[off - 1, at], t1r.at[off - 1, at], t1_send.at[off - 1, slot], t1_recv.at[off - 1, slot],
            col=(my_col + off) % cols,
        )

    def keep(n, slot):
        return gt.at[n // 2, pl.ds(pl.multiple_of(n % 2 * rows + slot * unit_rows, unit_rows), unit_rows)]

    def first_terms(d):
        for da in sides_of(d):
            for db in range(1 - b_side, b_side):
                @pl.when(both_inside(da, db))
                def _():
                    for k in range(4):
                        sibling_copy(da, db, k).wait_recv()

        def one_side(s, carry):
            plane = here["a"] + d * (1 - 2 * s)

            @pl.when(jnp.logical_and(plane >= 0, plane < a_side))
            def _():
                for g in range(b_side // unit):
                    chunk = plane * (b_side // unit) + g
                    first_chip = chunk * unit
                    off = (first_chip // share - my_col + cols) % cols
                    slot = first_chip % share // unit

                    def body(n, carry):
                        left_side = e2x[pl.ds(first_chip, unit)].reshape(unit_rows, fj)
                        part = gb[pl.ds(pl.multiple_of(n * TILE, TILE), TILE), :]
                        terms = lax.dot_general(
                            left_side, part, (((1,), (1,)), ((), ())), preferred_element_type=f32
                        )

                        @pl.when(off == 0)
                        def _():
                            keep(n, slot)[...] = terms

                        @pl.when(off != 0)
                        def _():
                            at = pl.ds(pl.multiple_of(slot * unit_rows, unit_rows), unit_rows)
                            to = pl.ds(pl.multiple_of(n * TILE, TILE), TILE)
                            t1s[off - 1, at, to] = terms.astype(bf16)

                        return carry

                    lax.fori_loop(0, fi // TILE, body, 0)

                    @pl.when(off != 0)
                    def _():
                        t1_copy(off, slot).start()

            return carry

        lax.fori_loop(0, 2 if d else 1, one_side, 0)

    ready = 0
    for kind, d, side, k in STEPS:
        if kind == OWN:
            own_terms(k)
        elif kind == OTHER:
            for q in (0,) if d == 0 else range(1, parts):
                other_terms(q, k)
        elif kind == GATHER:
            gather(d, side, k)
        elif kind == SUMS:
            for q in range(ready, 1 if d == a_side - 1 else parts):
                terms_ready(q)
                ready = q + 1
            send_sums(d, side, k)
        else:
            first_terms(d)

    def last_wait(kept):
        for da in range(1 - a_side, a_side):
            for db in range(1 - b_side, b_side):
                for k in range(4):
                    axis, _ = way_out(da, db, k)
                    recent = abs(da) == 1 and axis == "a" or da == 0
                    if recent == kept and (da, db) != (0, 0):
                        @pl.when(both_inside(da, db))
                        def _():
                            sum_copy(da, db, k).wait_send()

    for da in range(1 - a_side, a_side):
        for db in range(1 - b_side, b_side):
            @pl.when(both_inside(da, db))
            def _():
                for k in range(4):
                    for way in onward(da, db, k):
                        @pl.when(inside(*WAYS[way]))
                        def _():
                            block_copy(da, db, k, way).wait_send()
                    sibling_copy(da, db, k).wait_send()
    for off in range(cols):
        for q in range(parts if off else 1):
            for h in range(2):
                d2d_copy(off, q, h).wait_send()
    for off in range(1, cols):
        for q in range(parts):
            e1_copy(off, q).wait_send()
    last_wait(False)

    for off in range(1, cols):
        for slot in range(share // unit):
            t1_copy(off, slot).wait_recv()

    def out_body(n, carry):
        at = pl.ds(pl.multiple_of(n * TILE, TILE), TILE)
        for slot in range(share // unit):
            these = pl.ds(slot * unit_rows, unit_rows)
            total = keep(n, slot)[...]
            for off in range(1, cols):
                total += t1r[off - 1, these, at].astype(f32)
            o1_ref[these, at] = total.astype(bf16)
        return carry

    lax.fori_loop(0, fi // TILE, out_body, 0)

    outputs = [pltpu.make_async_copy(o1_ref, o1_hbm, out_sem.at[4])]
    outputs[0].start()
    for k in late + near:
        o2_ref[:, piece(k)] = sum_of(0, 0, k)
        outputs.append(pltpu.make_async_copy(o2_ref.at[:, piece(k)], o2_hbm.at[:, piece(k)], out_sem.at[k]))
        outputs[-1].start()

    last_wait(True)
    for off in range(1, cols):
        for slot in range(share // unit):
            t1_copy(off, slot).wait_send()
    for copy in outputs:
        copy.wait()


def hand_on(cuts_of, *refs):
    count = len(cuts_of)
    sources, targets, held = refs[:count], refs[count : 2 * count], refs[2 * count : 3 * count]
    in_sem, out_sem = refs[3 * count :]
    reads, writes = [], []
    for i, pieces_of in enumerate(cuts_of):
        step = sources[i].shape[0] // pieces_of
        for n in range(pieces_of):
            at = pl.ds(n * step, step)
            sems = in_sem.at[len(reads)], out_sem.at[len(reads)]
            reads.append(pltpu.make_async_copy(sources[i].at[at], held[i].at[at], sems[0]))
            writes.append(pltpu.make_async_copy(held[i].at[at], targets[i].at[at], sems[1]))
    for copy in reads:
        copy.start()
    for read, write in zip(reads, writes):
        read.wait()
        write.start()
    for copy in writes:
        copy.wait()


def local(rows_size, cols, e1, e2, g):
    chips = rows_size // 2
    a_side = 4
    b_side = chips // a_side
    block, fj = e2.shape
    rows, fi = e1.shape
    bf16 = jnp.bfloat16
    hbm = pl.BlockSpec(memory_space=pl.ANY)
    dma = pltpu.SemaphoreType.DMA
    pieces = cuts(fj)
    share = chips // cols
    parts, slots = max(share // b_side, 1), share // min(share, b_side)
    short, long = 2 * pieces[0][2], 2 * pieces[2][2]
    short_slots = b_side * slots_of(a_side) + slots_of(b_side)
    long_slots = a_side * slots_of(b_side) + slots_of(a_side)
    shapes = jax.ShapeDtypeStruct(e1.shape, bf16), jax.ShapeDtypeStruct(e2.shape, bf16)
    grads = pl.pallas_call(
        functools.partial(kernel, a_side, b_side, cols),
        out_shape=shapes,
        in_specs=[hbm, hbm, hbm],
        out_specs=(hbm, hbm),
        scratch_shapes=[
            pltpu.VMEM((rows, fi), bf16),
            pltpu.VMEM((block, fj), bf16),
            pltpu.VMEM((rows, fi), bf16),
            pltpu.VMEM((cols - 1, rows, fi), bf16),
            pltpu.VMEM((chips, 2, block, fj), bf16),
            pltpu.VMEM((fi, fj), bf16),
            pltpu.VMEM((chips, 2, block, fj), bf16),
            pltpu.VMEM((chips, block, fj), bf16),
            pltpu.VMEM((short_slots, block, short), bf16),
            pltpu.VMEM((long_slots, block, long), bf16),
            pltpu.VMEM((block, max(short, long) // 2), jnp.float32),
            pltpu.VMEM((cols - 1, rows, fi), bf16),
            pltpu.VMEM((cols - 1, rows, fi), bf16),
            pltpu.VMEM((SLOTS, fi, TILE), jnp.float32),
            dma((2,)), dma((5,)), dma((SLOTS,)),
            dma((cols - 1, parts)), dma((cols - 1, parts)),
            dma((chips, 4, 4)), dma((chips, 4)),
            dma((chips, 4)), dma((chips, 4)),
            dma((cols, parts, 2)), dma((cols, parts, 2)),
            dma((chips, 4)), dma((short_slots, 2)), dma((long_slots, 2)),
            dma((cols - 1, slots)), dma((cols - 1, slots)),
        ],
        compiler_params=pltpu.CompilerParams(
            collective_id=0, has_side_effects=True, vmem_limit_bytes=67043328
        ),
    )(e1, e2, g)
    cuts_of = 4, block // 16
    return pl.pallas_call(
        functools.partial(hand_on, cuts_of),
        out_shape=shapes,
        in_specs=[hbm, hbm],
        out_specs=(hbm, hbm),
        scratch_shapes=[pltpu.VMEM(each.shape, bf16) for each in shapes] + [dma((sum(cuts_of),))] * 2,
    )(*grads)


def solution(mesh):
    return jax.shard_map(
        functools.partial(local, mesh.shape["row"], mesh.shape["col"]),
        mesh=mesh,
        in_specs=(P("col", "row"), P("row", "col"), P("row", "col")),
        out_specs=(P("col", "row"), P("row", "col")),
        check_vma=False,
    )
```

```python
import functools

import jax
import jax.numpy as jnp
from jax import lax
from jax.experimental import pallas as pl
from jax.experimental.pallas import tpu as pltpu
from jax.sharding import PartitionSpec as P

OWN, OTHER, GATHER, SUMS, FIRST = range(5)
STEPS = (
    (OWN, 0, 0, 0), (GATHER, 0, 1, 0), (OWN, 0, 0, 1), (GATHER, 1, 0, 2), (GATHER, 0, 1, 1), (OTHER, 0, 0, 0),
    (OTHER, 0, 0, 1), (GATHER, 0, 1, 2), (GATHER, 1, 0, 3), (SUMS, 3, 0, 0), (SUMS, 3, 1, 2), (SUMS, 3, 1, 1),
    (SUMS, 3, 0, 1), (GATHER, 1, 1, 2), (SUMS, 3, 1, 0), (GATHER, 1, 0, 1), (OTHER, 1, 0, 0),
    (GATHER, 0, 1, 3), (SUMS, 3, 1, 3), (OTHER, 1, 0, 1), (SUMS, 3, 0, 2), (GATHER, 2, 0, 2),
    (GATHER, 1, 1, 1), (GATHER, 1, 1, 3), (SUMS, 2, 1, 3), (GATHER, 2, 0, 3), (GATHER, 1, 0, 0),
    (SUMS, 3, 0, 3), (GATHER, 1, 1, 0), (SUMS, 1, 1, 3), (GATHER, 3, 0, 2), (SUMS, 2, 0, 1), (SUMS, 2, 1, 0),
    (SUMS, 2, 1, 1), (FIRST, 1, 0, 0), (SUMS, 2, 1, 2), (SUMS, 2, 0, 3), (GATHER, 2, 0, 0), (SUMS, 2, 0, 0),
    (GATHER, 2, 0, 1), (GATHER, 2, 1, 3), (FIRST, 0, 0, 0), (GATHER, 3, 0, 0), (GATHER, 2, 1, 2),
    (GATHER, 3, 0, 3), (GATHER, 2, 1, 0), (GATHER, 2, 1, 1), (SUMS, 1, 1, 2), (SUMS, 1, 1, 0),
    (GATHER, 3, 0, 1), (SUMS, 1, 1, 1), (GATHER, 3, 1, 2), (SUMS, 1, 0, 3), (FIRST, 2, 0, 0),
    (GATHER, 3, 1, 1), (SUMS, 2, 0, 2), (SUMS, 0, 1, 2), (SUMS, 1, 0, 0), (GATHER, 3, 1, 3),
    (GATHER, 3, 1, 0), (SUMS, 0, 1, 0), (SUMS, 0, 1, 3), (FIRST, 3, 0, 0), (SUMS, 1, 0, 2), (SUMS, 1, 0, 1),
    (SUMS, 0, 1, 1),
)
FIRST_SHARE = 0.4
TILE = 256
SLOTS = 11
BAND = 256


def cuts(fj):
    unit = fj // 256
    short = round(unit * FIRST_SHARE)
    widths = [(True, short), (True, short), (False, unit - short), (False, unit - short)]
    out, at = [], 0
    for kind, w in widths:
        out.append((kind, at, w * 128))
        at += w * 128
    return out


def chunks_of(fj):
    return min(16, fj // TILE)


def slots_of(side):
    return 1 if side == 2 else side + 1


def kernel(
    a_side, b_side, cols,
    e1_hbm, e2_hbm, g_ref, o1_ref, o2_ref,
    e1_ref, e1x, e2x, gb, p2, stage, s2, rb_short, rb_long, gt,
    free_sem, in_sem, g_sem, e1_send, e1_recv, ag_send, ag_recv, sib_send, sib_recv,
    d2d_send, d2d_recv, rs_send, rs_recv_short, rs_recv_long, t1_send, t1_recv,
):
    chips = a_side * b_side
    block, fj = e2_hbm.shape
    rows, fi = e1_hbm.shape
    share = chips // cols
    bf16, f32 = jnp.bfloat16, jnp.float32
    pieces, chunks = cuts(fj), chunks_of(fj)
    sides = {"a": a_side, "b": b_side}

    me = lax.axis_index("row")
    my_col = lax.axis_index("col")
    chip, core = me // 2, me % 2
    other = 1 - core
    here = {"a": chip // b_side, "b": chip % b_side}
    sibling = chip * 2 + other

    def at_offset(da, db):
        return chip + da * b_side + db

    def neighbour(axis, sign):
        return (chip + sign * (b_side if axis == "a" else 1)) * 2 + core

    def inside(axis, d):
        where = here[axis] + d
        return jnp.logical_and(where >= 0, where < sides[axis])

    def both_inside(da, db):
        return jnp.logical_and(inside("a", da), inside("b", db))

    def piece(k):
        return pl.ds(pieces[k][1], pieces[k][2])

    def remote(src, dst, send, recv, **to):
        return pltpu.make_async_remote_copy(
            src_ref=src, dst_ref=dst, send_sem=send, recv_sem=recv,
            device_id=to, device_id_type=pl.DeviceIdType.MESH,
        )

    WAYS = (("a", 1), ("a", -1), ("b", 1), ("b", -1))

    e2_load = pltpu.make_async_copy(e2_hbm, e2x.at[chip, core], in_sem.at[0])
    e1_loads = [
        pltpu.make_async_copy(
            e1_hbm.at[pl.ds((2 * c + half) * block, block)], e1_ref.at[0, c, half], in_sem.at[1 + 2 * c + half]
        )
        for c in range(share)
        for half in range(2)
    ]
    for copy in [e2_load] + e1_loads:
        copy.start()

    barrier = pltpu.get_barrier_semaphore()
    for axis, sign in WAYS:
        @pl.when(inside(axis, sign))
        def _():
            pl.semaphore_signal(
                barrier, inc=1, device_id={"row": neighbour(axis, sign)}, device_id_type=pl.DeviceIdType.MESH
            )
    pl.semaphore_signal(barrier, inc=1, device_id={"row": sibling}, device_id_type=pl.DeviceIdType.MESH)
    for off in range(1, cols):
        pl.semaphore_signal(
            barrier, inc=1, device_id={"col": (my_col + off) % cols}, device_id_type=pl.DeviceIdType.MESH
        )
    peers = sum(inside(*way).astype(jnp.int32) for way in WAYS)
    pl.semaphore_wait(barrier, peers + cols)

    def block_copy(da, db, k, way):
        src_chip = at_offset(da, db)
        dst = e2x.at[src_chip, core, :, piece(k)]
        return remote(
            dst, dst, ag_send.at[src_chip, k, way], ag_recv.at[src_chip, k], row=neighbour(*WAYS[way])
        )

    def sibling_copy(da, db, k):
        src_chip = at_offset(da, db)
        dst = e2x.at[src_chip, core, :, piece(k)]
        return remote(dst, dst, sib_send.at[src_chip, k], sib_recv.at[src_chip, k], row=sibling)

    def onward(da, db, k):
        first, second = ("b", "a") if pieces[k][0] else ("a", "b")
        d = {"a": da, "b": db}
        for way, (axis, sign) in enumerate(WAYS):
            if axis == second:
                if d[second] * sign <= 0:
                    yield way
            elif d[second] == 0 and d[first] * sign <= 0:
                yield way

    def send_on(da, db, k):
        for way in onward(da, db, k):
            @pl.when(inside(*WAYS[way]))
            def _():
                block_copy(da, db, k, way).start()

    near, late = (0, 1), (2, 3)

    def sides_of(d):
        return (d, -d) if d else (0,)

    def gather(d, side, k):
        for db in across if side else (0,):
            for da in sides_of(d):
                @pl.when(both_inside(da, db))
                def _():
                    block_copy(da, db, k, 0).wait_recv()
                    send_on(da, db, k)
                    sibling_copy(da, db, k).start()

    across = sorted((db for db in range(1 - b_side, b_side) if db), key=abs)

    e2_load.wait()
    for k in late + near:
        for way in onward(0, 0, k):
            if WAYS[way][0] == "a":
                @pl.when(inside(*WAYS[way]))
                def _():
                    block_copy(0, 0, k, way).start()
    for k in near + late:
        for way in onward(0, 0, k):
            if WAYS[way][0] == "b":
                @pl.when(inside(*WAYS[way]))
                def _():
                    block_copy(0, 0, k, way).start()

    unit = min(share, b_side)
    unit_rows = unit * 2 * block
    parts = max(share // b_side, 1)
    part_chips = share // parts

    def part_of(col, q):
        return jnp.where(col * 2 < cols, q, parts - 1 - q)

    def e1_copy(off, q):
        at = pl.ds(part_of(my_col, q) * part_chips, part_chips)
        return remote(
            e1_ref.at[0, at], e1x.at[off - 1, at], e1_send.at[off - 1, q], e1_recv.at[off - 1, q],
            col=(my_col + off) % cols,
        )

    def e1_arrival(off, q):
        from_col = (my_col - off + cols) % cols
        at = pl.ds(part_of(from_col, q) * part_chips, part_chips)
        return remote(
            e1_ref.at[0, at], e1x.at[off - 1, at], e1_send.at[off - 1, q], e1_recv.at[off - 1, q], col=from_col
        )

    for copy in e1_loads:
        copy.wait()
    for q in range(parts):
        for off in range(1, cols):
            e1_copy(off, q).start()

    bands = fi // BAND

    def load(m):
        n, at = m // bands, m % bands
        return pltpu.make_async_copy(
            g_ref.at[pl.ds(pl.multiple_of(at * BAND, BAND), BAND), pl.ds(pl.multiple_of(n * TILE, TILE), TILE)],
            gt.at[m % SLOTS], g_sem.at[m % SLOTS],
        )

    tiles = fj // TILE
    for n in range(SLOTS):
        load(n).start()
    for k in near + late:
        sibling_copy(0, 0, k).start()

    span = fj // chunks
    wide = min(2 * TILE, span)

    def ordered(ref, count):
        mine = ref[:, core].reshape(count * block, fi)
        return jnp.concatenate([mine, ref[:, other].reshape(count * block, fi)], axis=0)

    def stage_slot(count, c):
        return c % 2, pl.ds(c // 2 % (share // count) * count, count)

    def put(terms, to, count, c, n, width):
        at = pl.ds(pl.multiple_of(c * span + n * width, width), width)
        within = pl.ds(pl.multiple_of(n * width, width), width)
        half = count * block
        p2[to, :, at] = terms[:half].reshape(count, block, width)
        slot, chips_at = stage_slot(count, c)
        stage[slot, chips_at, :, within] = terms[half:].reshape(count, block, width)

    def group_of(off, q):
        return 1 + q * (cols - 1) + off - 1 if off else 0

    def d2d_copy(off, q, c):
        from_col = (my_col - off + cols) % cols
        count = part_chips if off else share
        first = from_col * share + (part_of(from_col, q) * part_chips if off else 0)
        group = group_of(off, q)
        slot, chips_at = stage_slot(count, c)
        return remote(
            stage.at[slot, chips_at],
            s2.at[pl.ds(first, count), :, pl.ds(pl.multiple_of(c * span, span), span)],
            d2d_send.at[group, c], d2d_recv.at[group, c], row=sibling,
        )

    last_sent = []

    def chunk_loop(off, q, h, fill):
        half = chunks // 2
        depth = 2 * parts if off else 2
        before = list(last_sent)

        def body(i, carry):
            c = h * half + i
            for copy in before:
                @pl.when(i < copy[3])
                def _():
                    d2d_copy(copy[0], copy[1], copy[2] + i).wait_send()

            @pl.when(i >= depth)
            def _():
                d2d_copy(off, q, c - depth).wait_send()

            fill(c)
            d2d_copy(off, q, c).start()
            return carry

        lax.fori_loop(0, half, body, 0)
        last_sent[:] = [(off, q, h * half + half - depth, depth)]

    def own_terms(h):
        to = pl.ds(my_col * share, share)

        def fill(c):
            def tile(i, carry):
                n = c * (span // TILE) + i
                lows = []
                for r in range(bands):
                    m = n * bands + r
                    load(m).wait()
                    lows.append(gt[m % SLOTS].astype(bf16))
                    gb[pl.ds(r * BAND, BAND), pl.ds(pl.multiple_of(n * TILE, TILE), TILE)] = lows[-1]

                    @pl.when(m + SLOTS < tiles * bands)
                    def _():
                        load(m + SLOTS).start()

                low = jnp.concatenate(lows, axis=0)
                terms = jnp.dot(ordered(e1_ref.at[0], share), low, preferred_element_type=f32).astype(bf16)
                put(terms, to, share, c, i, TILE)
                return carry

            lax.fori_loop(0, span // TILE, tile, 0)

        chunk_loop(0, 0, h, fill)

    def other_terms(q, h):
        for off in range(1, cols):
            if h == 0:
                e1_arrival(off, q).wait_recv()
            from_col = (my_col - off + cols) % cols
            first = part_of(from_col, q) * part_chips
            to = pl.ds(from_col * share + first, part_chips)

            def fill(c):
                def tile(m, carry):
                    at = pl.ds(pl.multiple_of(c * span + m * wide, wide), wide)
                    left = ordered(e1x.at[off - 1, pl.ds(first, part_chips)], part_chips)
                    terms = jnp.dot(left, gb[:, at], preferred_element_type=f32).astype(bf16)
                    put(terms, to, part_chips, c, m, wide)
                    return carry

                lax.fori_loop(0, span // wide, tile, 0)

            chunk_loop(off, q, h, fill)

    def terms_ready(q):
        for off in range(0 if q == 0 else 1, cols):
            def body(c, carry):
                d2d_copy(off, q, c).wait_recv()
                return carry

            lax.fori_loop(0, chunks, body, 0)

    def sum_slot(k, axis, sign, to):
        short = pieces[k][0]
        first, second = ("a", "b") if short else ("b", "a")
        place = to["a"] if axis == "a" else to["b"]
        slot = 0 if sides[axis] == 2 else (place + 1 if sign > 0 else place)
        if axis == first:
            slot = to[second] * slots_of(sides[first]) + slot
        else:
            slot = sides[second] * slots_of(sides[first]) + slot
        start = pieces[k][1] if short else pieces[k][1] - pieces[2][1]
        buf = rb_short if short else rb_long
        sem = rs_recv_short if short else rs_recv_long
        return buf.at[slot, :, pl.ds(start, pieces[k][2])], sem.at[slot, k % 2]

    def place_of(da, db):
        return {"a": here["a"] + da, "b": here["b"] + db}

    def way_out(da, db, k):
        first, second = ("a", "b") if pieces[k][0] else ("b", "a")
        d = {"a": da, "b": db}
        axis = first if d[first] else second
        return axis, (1 if d[axis] > 0 else -1)

    def sum_copy(da, db, k):
        axis, sign = way_out(da, db, k)
        to_chip = at_offset(da, db)
        dst, sem = sum_slot(k, axis, sign, place_of(da, db))
        return remote(
            p2.at[to_chip, :, piece(k)], dst, rs_send.at[to_chip, k], sem, row=neighbour(axis, sign)
        )

    def arrivals(da, db, k):
        first, second = ("a", "b") if pieces[k][0] else ("b", "a")
        d = {"a": da, "b": db}
        out = []
        for sign in (1, -1):
            if d[first] * sign >= 0:
                out.append((first, sign))
        if d[first] == 0:
            for sign in (1, -1):
                if d[second] * sign >= 0:
                    out.append((second, sign))
        return out

    def kept(k, n):
        width = min(TILE, pieces[k][2] - n * TILE)
        return gt.at[n, pl.ds(unit_rows, block), pl.ds(0, width)], pl.ds(n * TILE, width)

    def sum_of(da, db, k, out):
        start, width = pieces[k][1:]
        to_chip = at_offset(da, db)
        strips = [kept(k, n) for n in range(-(-width // TILE))]
        for strip, at in strips:
            whole_at = pl.ds(start + at.start, at.size)
            strip[...] = p2[to_chip, :, whole_at].astype(f32) + s2[to_chip, :, whole_at].astype(f32)
        for axis, sign in arrivals(da, db, k):
            @pl.when(inside(axis, -sign))
            def _():
                buf, sem = sum_slot(k, axis, sign, place_of(da, db))
                remote(buf, buf, rs_send.at[0, k], sem, row=sibling).wait_recv()
                for strip, at in strips:
                    strip[...] += buf[:, at].astype(f32)
        for strip, at in strips:
            out[:, pl.ds(start + at.start, at.size)] = strip[...].astype(bf16)

    def send_sums(d, side, k):
        for db in reversed(across) if side else (0,):
            for da in sides_of(d):
                @pl.when(both_inside(da, db))
                def _():
                    sum_of(da, db, k, p2.at[at_offset(da, db)])
                    sum_copy(da, db, k).start()


    def t1_copy(off, slot):
        at = pl.ds(slot * unit, unit)
        return remote(
            e1_ref.at[off - 1, at], e1x.at[off - 1, at], t1_send.at[off - 1, slot], t1_recv.at[off - 1, slot],
            col=(my_col + off) % cols,
        )

    def keep(n, slot):
        return gt.at[n * (share // unit) + slot, pl.ds(0, unit_rows)]

    def first_terms(d):
        for da in sides_of(d):
            for db in range(1 - b_side, b_side):
                @pl.when(both_inside(da, db))
                def _():
                    for k in range(4):
                        sibling_copy(da, db, k).wait_recv()

        def one_side(s, carry):
            plane = here["a"] + d * (1 - 2 * s)

            @pl.when(jnp.logical_and(plane >= 0, plane < a_side))
            def _():
                for g in range(b_side // unit):
                    chunk = plane * (b_side // unit) + g
                    first_chip = chunk * unit
                    off = (first_chip // share - my_col + cols) % cols
                    slot = first_chip % share // unit

                    def body(n, carry):
                        left_side = e2x[pl.ds(first_chip, unit)].reshape(unit_rows, fj)
                        part = gb[pl.ds(pl.multiple_of(n * TILE, TILE), TILE), :]
                        terms = lax.dot_general(
                            left_side, part, (((1,), (1,)), ((), ())), preferred_element_type=f32
                        )

                        @pl.when(off == 0)
                        def _():
                            keep(n, slot)[...] = terms

                        @pl.when(off != 0)
                        def _():
                            to = pl.ds(pl.multiple_of(n * TILE, TILE), TILE)
                            low = terms.astype(bf16).reshape(unit, 2, block, TILE)
                            e1_ref[off - 1, pl.ds(slot * unit, unit), :, :, to] = low

                        return carry

                    lax.fori_loop(0, fi // TILE, body, 0)

                    @pl.when(off != 0)
                    def _():
                        t1_copy(off, slot).start()

            return carry

        lax.fori_loop(0, 2 if d else 1, one_side, 0)

    def let_terms_in():
        for off in range(1, cols):
            for q in range(parts):
                e1_copy(off, q).wait_send()
            pl.semaphore_signal(
                free_sem, inc=1, device_id={"col": (my_col + off) % cols}, device_id_type=pl.DeviceIdType.MESH
            )
        pl.semaphore_wait(free_sem, cols - 1)

    ready, open_to_terms = 0, False
    for kind, d, side, k in STEPS:
        if kind == OWN:
            own_terms(k)
        elif kind == OTHER:
            for q in (0,) if d == 0 else range(1, parts):
                other_terms(q, k)
        elif kind == GATHER:
            gather(d, side, k)
        elif kind == SUMS:
            for q in range(ready, 1 if d == a_side - 1 else parts):
                terms_ready(q)
                ready = q + 1
            send_sums(d, side, k)
        else:
            if not open_to_terms:
                let_terms_in()
                open_to_terms = True
            first_terms(d)

    def last_wait(kept):
        for da in range(1 - a_side, a_side):
            for db in range(1 - b_side, b_side):
                for k in range(4):
                    axis, _ = way_out(da, db, k)
                    recent = abs(da) == 1 and axis == "a" or da == 0
                    if recent == kept and (da, db) != (0, 0):
                        @pl.when(both_inside(da, db))
                        def _():
                            sum_copy(da, db, k).wait_send()

    for da in range(1 - a_side, a_side):
        for db in range(1 - b_side, b_side):
            @pl.when(both_inside(da, db))
            def _():
                for k in range(4):
                    for way in onward(da, db, k):
                        @pl.when(inside(*WAYS[way]))
                        def _():
                            block_copy(da, db, k, way).wait_send()
                    sibling_copy(da, db, k).wait_send()
    for off, q, c, depth in last_sent:
        for i in range(depth):
            d2d_copy(off, q, c + i).wait_send()
    last_wait(False)

    for off in range(1, cols):
        for slot in range(share // unit):
            t1_copy(off, slot).wait_recv()

    def out_body(n, carry):
        at = pl.ds(pl.multiple_of(n * TILE, TILE), TILE)
        for slot in range(share // unit):
            these = pl.ds(slot * unit_rows, unit_rows)
            total = keep(n, slot)[...]
            for off in range(1, cols):
                total += e1x[off - 1, pl.ds(slot * unit, unit), :, :, at].reshape(unit_rows, TILE).astype(f32)
            o1_ref[these, at] = total.astype(bf16)
        return carry

    lax.fori_loop(0, fi // TILE, out_body, 0)

    for k in late + near:
        sum_of(0, 0, k, o2_ref)

    last_wait(True)
    for off in range(1, cols):
        for slot in range(share // unit):
            t1_copy(off, slot).wait_send()


def hand_on(first_ref, second_ref, first_out, second_out, sem):
    copies = (
        pltpu.make_async_copy(first_ref, first_out, sem.at[0]),
        pltpu.make_async_copy(second_ref, second_out, sem.at[1]),
    )
    for copy in copies:
        copy.start()
    for copy in copies:
        copy.wait()


def local(rows_size, cols, e1, e2, g):
    chips = rows_size // 2
    a_side = 4
    b_side = chips // a_side
    block, fj = e2.shape
    rows, fi = e1.shape
    bf16 = jnp.bfloat16
    vmem, hbm = pl.BlockSpec(memory_space=pltpu.VMEM), pl.BlockSpec(memory_space=pltpu.HBM)
    dma = pltpu.SemaphoreType.DMA
    pieces = cuts(fj)
    share = chips // cols
    parts, slots = max(share // b_side, 1), share // min(share, b_side)
    short, long = 2 * pieces[0][2], 2 * pieces[2][2]
    short_slots = b_side * slots_of(a_side) + slots_of(b_side)
    long_slots = a_side * slots_of(b_side) + slots_of(a_side)
    shapes = jax.ShapeDtypeStruct(e1.shape, bf16), jax.ShapeDtypeStruct(e2.shape, bf16)
    grads = pl.pallas_call(
        functools.partial(kernel, a_side, b_side, cols),
        out_shape=shapes,
        in_specs=[hbm, hbm, hbm],
        out_specs=(vmem, vmem),
        scratch_shapes=[
            pltpu.VMEM((cols - 1, share, 2, block, fi), bf16),
            pltpu.VMEM((cols - 1, share, 2, block, fi), bf16),
            pltpu.VMEM((chips, 2, block, fj), bf16),
            pltpu.VMEM((fi, fj), bf16),
            pltpu.VMEM((chips, block, fj), bf16),
            pltpu.VMEM((2, share, block, fj // chunks_of(fj)), bf16),
            pltpu.VMEM((chips, block, fj), bf16),
            pltpu.VMEM((short_slots, block, short), bf16),
            pltpu.VMEM((long_slots, block, long), bf16),
            pltpu.VMEM((SLOTS, BAND, TILE), jnp.float32),
            pltpu.SemaphoreType.REGULAR,
            dma((1 + 2 * share,)), dma((SLOTS,)),
            dma((cols - 1, parts)), dma((cols - 1, parts)),
            dma((chips, 4, 4)), dma((chips, 4)),
            dma((chips, 4)), dma((chips, 4)),
            dma((1 + parts * (cols - 1), chunks_of(fj))), dma((1 + parts * (cols - 1), chunks_of(fj))),
            dma((chips, 4)), dma((short_slots, 2)), dma((long_slots, 2)),
            dma((cols - 1, slots)), dma((cols - 1, slots)),
        ],
        compiler_params=pltpu.CompilerParams(
            collective_id=0, has_side_effects=True, vmem_limit_bytes=54935552
        ),
    )(e1, e2, g)
    return pl.pallas_call(
        hand_on,
        out_shape=shapes,
        in_specs=[vmem, vmem],
        out_specs=(hbm, hbm),
        scratch_shapes=[dma((2,))],
        compiler_params=pltpu.CompilerParams(vmem_limit_bytes=1 << 22),
    )(*grads)


def solution(mesh):
    return jax.shard_map(
        functools.partial(local, mesh.shape["row"], mesh.shape["col"]),
        mesh=mesh,
        in_specs=(P("col", "row"), P("row", "col"), P("row", "col")),
        out_specs=(P("col", "row"), P("row", "col")),
        check_vma=False,
    )
```
